256 devices in a mesh: grp: 4 (over y), seq: 64 (over x, z, core).
Axes of the slice: x: 4, y: 4, z: 8, core: 2. Of those that a mesh axis runs over, the one named last changes fastest.
Arguments:
- queries: bfloat16 [65536, 2048], P(('grp', 'seq')), may hold values from -48 to 48
- key_rows: bfloat16 [65536, 512], P(('grp', 'seq')), may hold values from -4.5 to 4.5
- value_rows: bfloat16 [65536, 512], P(('grp', 'seq')), may hold values from -6 to 6
- segments: int32 [65536], P(('grp', 'seq')), may hold values from 0 to 30, as said below
Outputs:
- attended: bfloat16 [65536, 2048], P(('grp', 'seq'))
- log_sums: float32 [16, 65536], P(None, ('grp', 'seq'))
The draws below stay inside these ranges and needn't reach their ends.
Inputs may be any that keep to these rules, and one draw needn't show every extreme that they name: `segments`: never falls along the sequence, starts at 0 and rises by one at each new document; the last token holds the largest value.
All inputs are finite; a program needn't handle non-finite values.
Results may differ from the reference program's by a relative error of at most 0.0035.
Values may be sent and summed in bfloat16 or wider, within the bound.
No kernel may reach another device: no remote copies, remote signals or barrier semaphores. Data moves between devices by JAX's collectives and lax.ppermute only.
A program may use at most 192 MiB of HBM per device.

```python
import math
import jax
import jax.numpy as jnp
from jax import lax

Q_HEADS = 16
KV_HEADS = 4
HEAD_DIM = 128
WINDOW = 4096
TOK_DEV = 256
SEQ_LEN = 65536


def boundary_flags(key):
    stretch = max(WINDOW // 2, 2)
    pieces = SEQ_LEN // stretch
    offsets = jax.random.randint(jax.random.fold_in(key, 11), (pieces,), 1, stretch)
    spots = jnp.arange(SEQ_LEN)
    first_mark = SEQ_LEN // 2 - TOK_DEV // 2
    second_mark = SEQ_LEN // 2 + TOK_DEV // 2
    low_piece = first_mark // stretch
    high_piece = min(pieces - 1, (second_mark + WINDOW) // stretch)
    piece_of = spots // stretch
    kept = (piece_of < low_piece) | (piece_of > high_piece)
    flags = (kept & (spots % stretch == offsets[piece_of])).astype(jnp.int32)
    flags = jnp.where((spots == first_mark) | (spots == second_mark), 1, flags)
    return flags.at[0].set(0)


def draw_segments(key, part):
    return jnp.cumsum(boundary_flags(key)).astype(jnp.int32)


def query_key_pair(key):
    group = Q_HEADS // KV_HEADS
    keys = jnp.clip(jax.random.normal(jax.random.fold_in(key, 21), (SEQ_LEN, KV_HEADS, HEAD_DIM), jnp.float32), -4.5, 4.5)
    queries = jnp.clip(3.0 * jax.random.normal(jax.random.fold_in(key, 22), (SEQ_LEN, KV_HEADS, group, HEAD_DIM), jnp.float32), -18.0, 18.0)
    return (queries.reshape(SEQ_LEN, Q_HEADS * HEAD_DIM).astype(jnp.bfloat16), keys.reshape(SEQ_LEN, KV_HEADS * HEAD_DIM).astype(jnp.bfloat16))


def draw_queries(key, part):
    return query_key_pair(key)[0]


def draw_key_rows(key, part):
    return query_key_pair(key)[1]


def steps_of(rng, extent, split, least, top_value):
    gain, own = 1.0, jax.random.fold_in(rng, 6)
    for position, blocks in split:
        heights = jnp.exp(jax.random.uniform(jax.random.fold_in(own, position), (blocks,), jnp.float32, least / len(split), top_value / len(split)))
        gain = gain * jnp.repeat(heights, extent[position] // blocks).reshape([-1 if axis == position else 1 for axis in range(len(extent))])
    return gain


def centred(key, dims, deviation, bound, cuts=(), kind=jnp.bfloat16):
    entries = jax.random.normal(key, dims, jnp.float32) * deviation
    if len(cuts) > 0:
        entries = steps_of(key, dims, cuts, -0.22, 0.18) * entries
    return jnp.clip(entries, min=-bound, max=bound).astype(kind)


def setup_inputs(seed: int = 0) -> dict:
    splits = jax.random.split(jax.random.key(seed), 5)
    return {
        "queries": draw_queries(jax.random.fold_in(splits[4], 71), 0),
        "key_rows": draw_key_rows(jax.random.fold_in(splits[4], 71), 0),
        "value_rows": centred(splits[2], (SEQ_LEN, KV_HEADS * HEAD_DIM), 1.0, 6.0, ((0, 256),)),
        "segments": draw_segments(jax.random.fold_in(splits[4], 71), 0),
    }


def reference(queries, key_rows, value_rows, segments):
    group = Q_HEADS // KV_HEADS
    block = math.gcd(SEQ_LEN, 512)
    count = SEQ_LEN // block
    span = block + WINDOW
    scale = 1.0 / math.sqrt(HEAD_DIM)
    width = KV_HEADS * HEAD_DIM
    key_pad = jnp.concatenate([jnp.zeros((WINDOW, width), key_rows.dtype), key_rows], axis=0)
    value_pad = jnp.concatenate([jnp.zeros((WINDOW, width), value_rows.dtype), value_rows], axis=0)
    seg_pad = jnp.concatenate([jnp.full((WINDOW,), -1, jnp.int32), segments.astype(jnp.int32)], axis=0)

    def one_block(index):
        first = (index * block).astype(jnp.int32)
        q_part = lax.dynamic_slice_in_dim(queries, first, block, 0).reshape(block, KV_HEADS, group, HEAD_DIM).astype(jnp.float32)
        k_part = lax.dynamic_slice_in_dim(key_pad, first, span, 0).reshape(span, KV_HEADS, HEAD_DIM).astype(jnp.float32)
        v_part = lax.dynamic_slice_in_dim(value_pad, first, span, 0).reshape(span, KV_HEADS, HEAD_DIM).astype(jnp.float32)
        q_seg = lax.dynamic_slice_in_dim(segments.astype(jnp.int32), first, block, 0)
        k_seg = lax.dynamic_slice_in_dim(seg_pad, first, span, 0)
        q_pos = first + jnp.arange(block, dtype=jnp.int32)
        k_pos = first - WINDOW + jnp.arange(span, dtype=jnp.int32)
        allowed = (k_pos[None, :] <= q_pos[:, None]) & (k_pos[None, :] > q_pos[:, None] - WINDOW) & (k_seg[None, :] == q_seg[:, None])
        scores = jnp.einsum('tkgd,lkd->kgtl', q_part, k_part, precision=lax.Precision.HIGHEST) * scale
        masked = jnp.where(allowed, scores, -1e+30)
        top = lax.optimization_barrier(jnp.max(masked, axis=-1))
        expo = jnp.where(allowed, jnp.exp(masked - top[..., None]), 0.0)
        total = lax.optimization_barrier(jnp.sum(expo, axis=-1))
        weights = lax.optimization_barrier(expo.astype(jnp.bfloat16))
        summed = jnp.einsum('kgtl,lkd->tkgd', weights.astype(jnp.float32), v_part, precision=lax.Precision.HIGHEST)
        out = summed / jnp.transpose(total, (2, 0, 1))[..., None]
        out = out.reshape(block, Q_HEADS * HEAD_DIM).astype(jnp.bfloat16)
        sums = (top + jnp.log(total)).reshape(Q_HEADS, block)
        return (out, sums)
    outs, sums = lax.map(one_block, jnp.arange(count, dtype=jnp.int32))
    attended = outs.reshape(SEQ_LEN, Q_HEADS * HEAD_DIM)
    log_sums = jnp.transpose(sums, (1, 0, 2)).reshape(Q_HEADS, SEQ_LEN)
    return (attended, log_sums)
```

```python
import math

import jax
import jax.numpy as jnp
from jax import lax
from jax.experimental import pallas as pl
from jax.experimental.pallas import tpu as pltpu
from jax.sharding import Mesh
from jax.sharding import PartitionSpec as P

Q_HEADS = 16
KV_HEADS = 4
HEAD_DIM = 128
WINDOW = 4096
TOK = 256
MY_Q = 8
GROUP = 4
HALF_Q = MY_Q * HEAD_DIM
HALF_KV = 2 * HEAD_DIM
MSG_ROWS = TOK + 8
GRP_SEQ = ("grp", "seq_0", "seq_1", "seq_2")
N_DEV = 256
SCALE = math.log2(math.e) / math.sqrt(HEAD_DIM)
LN2 = math.log(2.0)
NEG = -1e30
ITEMS = 2 * MY_Q
IN_VMEM = pl.BlockSpec(memory_space=pltpu.VMEM)
LEAN = pltpu.CompilerParams(vmem_limit_bytes=16 << 20)
FAR = 1 << 20


def pack_kernel(core_ref, k_ref, v_ref, seg_ref, same_ref, cross_ref):
    core = core_ref[0]
    seg = jnp.broadcast_to(seg_ref[...].astype(jnp.float32), (8, TOK)).astype(jnp.bfloat16)
    seg = jnp.concatenate([seg, seg], axis=1)
    same_ref[TOK:, :] = seg
    cross_ref[TOK:, :] = seg
    for e in range(2):

        @pl.when(core == e)
        def _():
            for ref, h in ((same_ref, e), (cross_ref, 1 - e)):
                ref[:TOK, :HALF_KV] = k_ref[:, h * HALF_KV : (h + 1) * HALF_KV]
                ref[:TOK, HALF_KV:] = v_ref[:, h * HALF_KV : (h + 1) * HALF_KV]


def pack(core, keys, values, segments):
    msg = jax.ShapeDtypeStruct((MSG_ROWS, 2 * HALF_KV), jnp.bfloat16)
    return pl.pallas_call(
        pack_kernel,
        grid_spec=pltpu.PrefetchScalarGridSpec(
            num_scalar_prefetch=1,
            grid=(1,),
            in_specs=[
                pl.BlockSpec((TOK, 512), lambda i, s: (0, 0)),
                pl.BlockSpec((TOK, 512), lambda i, s: (0, 0)),
                pl.BlockSpec((1, TOK), lambda i, s: (0, 0)),
            ],
            out_specs=[
                pl.BlockSpec((MSG_ROWS, 512), lambda i, s: (0, 0)),
                pl.BlockSpec((MSG_ROWS, 512), lambda i, s: (0, 0)),
            ],
        ),
        out_shape=(msg, msg),
        name="pack",
    )(core, keys, values, segments)


def hold(array):
    return pltpu.with_memory_space_constraint(array, pltpu.VMEM)


def rows_to_cols(row):
    return jnp.transpose(jnp.broadcast_to(row, (128, TOK)))


def split_kernel(q_own, q_sib, out_ref):
    for i in range(ITEMS):
        ref = (q_own, q_sib)[i % 2]
        q = ref[:, i // 2 * 128 : (i // 2 + 1) * 128].astype(jnp.float32) * SCALE
        hi = q.astype(jnp.bfloat16)
        out_ref[i, :, :128] = hi
        out_ref[i, :, 128:] = (q - hi.astype(jnp.float32)).astype(jnp.bfloat16)


def split_queries(q_own, q_sib):
    return pl.pallas_call(
        split_kernel,
        in_specs=[IN_VMEM] * 2,
        out_specs=IN_VMEM,
        out_shape=pltpu.VMEM((ITEMS, TOK, 256), jnp.bfloat16),
        compiler_params=LEAN,
        name="split_queries",
    )(hold(q_own), hold(q_sib))


def attend_kernel(back, init, final, *refs):
    n = 2 * len(back)
    refs = list(refs)
    place_ref, q_ref = refs.pop(0), refs.pop(0)
    qmsg_refs = [refs.pop(0), refs.pop(0)]
    kv_refs = [refs.pop(0) for _ in range(n)]
    if not init:
        m_in, acc_in = refs.pop(0), refs.pop(0)
    if final:
        o_refs = [refs.pop(0), refs.pop(0)]
        lse_refs = [refs.pop(0), refs.pop(0)]
    else:
        m_out, acc_out = refs.pop(0), refs.pop(0)
    s_ref, top_ref = refs

    chip, core = place_ref[0], place_ref[1]
    side = (1 - 2 * core) * TOK

    def seg_row(ref):
        return ref[TOK : TOK + 1, :TOK].astype(jnp.float32)

    def columns(ref, first, g):
        return ref[:TOK, pl.ds(pl.multiple_of(first + g * 128, 128), 128)]

    def score(i, half, masked):
        g = i // (2 * GROUP)
        q2 = q_ref[i]
        keys = jnp.concatenate([columns(r, 0, g) for r in kv_refs], axis=0)
        keys = jnp.concatenate([keys, keys], axis=1)
        s = lax.dot_general(q2, keys, (((1,), (1,)), ((), ())), preferred_element_type=jnp.float32)
        tiles = [s[:, t * 128 : (t + 1) * 128] for t in range(2 * n)]
        if masked:
            qseg = rows_to_cols(seg_row(qmsg_refs[half]))
            qi = lax.broadcasted_iota(jnp.int32, (TOK, 128), 0)
            kj = lax.broadcasted_iota(jnp.int32, (TOK, 128), 1)
            for t in range(2 * n):
                b = t // 2
                k = back[b // 2]
                delta = (b % 2 - half) * side - 512 * k + (t % 2) * 128
                delta = jnp.where(chip >= k, delta, FAR)
                dist = kj - qi + delta
                kseg = seg_row(kv_refs[b])[:, t % 2 * 128 : (t % 2 + 1) * 128]
                ok = (dist <= 0) & (dist > -WINDOW) & (kseg == qseg)
                tiles[t] = jnp.where(ok, tiles[t], NEG)
        top = tiles[0]
        for t in range(2 * n):
            s_ref[half, :, t * 128 : (t + 1) * 128] = tiles[t]
            if t:
                top = jnp.maximum(top, tiles[t])
        top_ref[half] = jnp.broadcast_to(jnp.max(top, axis=1, keepdims=True), (TOK, 128))

    def combine(i, half):
        g = i // (2 * GROUP)
        vals = jnp.concatenate([columns(r, HALF_KV, g) for r in kv_refs], axis=0)
        vals = jnp.concatenate([vals, jnp.ones_like(vals)], axis=1)
        top = top_ref[half]
        if init:
            m = top
        else:
            m_old = m_in[i]
            m = jnp.maximum(m_old, top)
        p = jnp.concatenate(
            [
                jnp.exp2(s_ref[half, :, t * 128 : (t + 1) * 128] - m).astype(jnp.bfloat16)
                for t in range(2 * n)
            ],
            axis=1,
        )
        acc = jnp.dot(p, vals, preferred_element_type=jnp.float32)
        if not init:
            fac = jnp.exp2(m_old - m)
            acc = acc_in[i] * jnp.concatenate([fac, fac], axis=1) + acc
        if final:
            h = i // 2
            total = acc[:, 128:]
            at = pl.ds(pl.multiple_of(h * 128, 128), 128)
            o_refs[half][:, at] = (acc[:, :128] / total).astype(jnp.bfloat16)
            lse = LN2 * (m + jnp.log2(total))
            lse_refs[half][pl.ds(h, 1), :] = jnp.transpose(lse)[:1, :]
        else:
            m_out[i] = m
            acc_out[i] = acc

    def run(masked):
        score(0, 0, masked)

        def body(j, _):
            i = 2 * j
            score(i + 1, 1, masked)
            combine(i, 0)
            score(jnp.minimum(i + 2, ITEMS - 2), 0, masked)
            combine(i + 1, 1)
            return 0

        lax.fori_loop(0, ITEMS // 2, body, 0)

    if min(back) > 0 and max(back) < 8:
        low = seg_row(kv_refs[0])
        for ref in kv_refs[1:]:
            low = jnp.minimum(low, seg_row(ref))
        high = jnp.maximum(seg_row(qmsg_refs[0]), seg_row(qmsg_refs[1]))
        whole = (jnp.min(low) == jnp.max(high)) & (chip >= max(back))
        pl.when(whole)(lambda: run(False))
        pl.when(jnp.logical_not(whole))(lambda: run(True))
    else:
        run(True)


def attend(place, q2, qmsg, kv, back, state, final):
    init = state is None
    args = [q2, *qmsg, *kv]
    if not init:
        args += list(state)
    if final:
        out_shape = [pltpu.VMEM((TOK, HALF_Q), jnp.bfloat16)] * 2
        out_shape += [pltpu.VMEM((MY_Q, TOK), jnp.float32)] * 2
    else:
        out_shape = [
            pltpu.VMEM((ITEMS, TOK, 128), jnp.float32),
            pltpu.VMEM((ITEMS, TOK, 256), jnp.float32),
        ]
    size = ITEMS * TOK * TOK * len(kv)
    return pl.pallas_call(
        lambda *refs: attend_kernel(back, init, final, *refs),
        in_specs=[pl.BlockSpec(memory_space=pltpu.SMEM)] + [IN_VMEM] * len(args),
        out_specs=[IN_VMEM] * len(out_shape),
        out_shape=out_shape,
        input_output_aliases={} if init or final else {len(args) - 1: 0, len(args): 1},
        scratch_shapes=[
            pltpu.VMEM((2, TOK, TOK * len(kv)), jnp.float32),
            pltpu.VMEM((2, TOK, 128), jnp.float32),
        ],
        cost_estimate=pl.CostEstimate(
            flops=size * 1024, transcendentals=size, bytes_accessed=0
        ),
        compiler_params=LEAN,
        name="attend_" + "_".join(map(str, back)),
    )(place, *map(hold, args))


def chips_on(by, cross=False):
    flip = 1 if cross else 0
    return [(d, (d + 2 * by) % N_DEV ^ flip) for d in range(N_DEV)]


def on_device(queries, key_rows, value_rows, segments):
    device = lax.axis_index(GRP_SEQ)
    core = device % 2
    chip = device // 2
    place = jnp.stack([chip, core]).astype(jnp.int32)
    swap = [(d, d ^ 1) for d in range(N_DEV)]

    def move(array, pairs):
        return lax.ppermute(array, GRP_SEQ, pairs)

    same, cross = pack(core[None].astype(jnp.int32), key_rows, value_rows, segments[None, :])
    fwd = [move(same, chips_on(1)), move(cross, chips_on(1, True))]
    bwd = [move(same, chips_on(8)), move(cross, chips_on(8, True))]
    sib = move(cross, swap)
    q_low, q_high = queries[:, :HALF_Q], queries[:, HALF_Q:]
    q_mine = jnp.where(core == 0, q_low, q_high)
    q_sib = move(jnp.where(core == 0, q_high, q_low), swap)
    q, qmsg = split_queries(q_mine, q_sib), [same, sib]

    state = attend(place, q, qmsg, [same, sib], (0,), None, False)
    for step in range(1, 5):
        if step < 4:
            fwd_next = [move(x, chips_on(1)) for x in fwd]
            bwd_next = [move(x, chips_on(-1)) for x in bwd]
        far = 8 if step == 1 else 9 - step
        state = attend(place, q, qmsg, [*fwd, *bwd], (step, far), state, step == 4)
        if step < 4:
            fwd, bwd = fwd_next, bwd_next

    o_mine, o_sib, l_mine, l_sib = state
    o_other = move(o_sib, swap)
    l_other = move(l_sib, swap)
    first = core == 0
    attended = jnp.concatenate(
        [jnp.where(first, o_mine, o_other), jnp.where(first, o_other, o_mine)], axis=1
    )
    log_sums = jnp.concatenate(
        [jnp.where(first, l_mine, l_other), jnp.where(first, l_other, l_mine)], axis=0
    )
    return (attended, log_sums)


def solution(mesh):
    split = Mesh(
        mesh.devices.reshape(mesh.shape["grp"], 4, 8, 2), ("grp", "seq_0", "seq_1", "seq_2")
    )
    placed = (P(GRP_SEQ, None), P(GRP_SEQ, None), P(GRP_SEQ, None), P(GRP_SEQ))
    return jax.shard_map(
        on_device,
        mesh=split,
        in_specs=placed,
        out_specs=(P(GRP_SEQ, None), P(None, GRP_SEQ)),
        check_vma=False,
    )
```

```python
import math

import jax
import jax.numpy as jnp
from jax import lax
from jax.experimental import pallas as pl
from jax.experimental.pallas import tpu as pltpu
from jax.sharding import Mesh
from jax.sharding import PartitionSpec as P

Q_HEADS = 16
KV_HEADS = 4
HEAD_DIM = 128
WINDOW = 4096
TOK = 256
MY_Q = 8
GROUP = 4
HALF_Q = MY_Q * HEAD_DIM
HALF_KV = 2 * HEAD_DIM
MSG_ROWS = TOK + 8
GRP_SEQ = ("grp", "seq_0", "seq_1", "seq_2")
N_DEV = 256
SCALE = math.log2(math.e) / math.sqrt(HEAD_DIM)
LN2 = math.log(2.0)
NEG = -1e30
LIMIT = 2.0**100
UNROLL = 4
ITEMS = 2 * MY_Q
IN_VMEM = pl.BlockSpec(memory_space=pltpu.VMEM)
LEAN = pltpu.CompilerParams(vmem_limit_bytes=16 << 20)
FAR = 1 << 20


def pack_kernel(core_ref, k_ref, v_ref, seg_ref, same_ref, cross_ref):
    core = core_ref[0]
    seg = jnp.broadcast_to(seg_ref[...].astype(jnp.float32), (8, TOK)).astype(jnp.bfloat16)
    seg = jnp.concatenate([seg, seg], axis=1)
    same_ref[TOK:, :] = seg
    cross_ref[TOK:, :] = seg
    for e in range(2):

        @pl.when(core == e)
        def _():
            for ref, h in ((same_ref, e), (cross_ref, 1 - e)):
                ref[:TOK, :HALF_KV] = k_ref[:, h * HALF_KV : (h + 1) * HALF_KV]
                ref[:TOK, HALF_KV:] = v_ref[:, h * HALF_KV : (h + 1) * HALF_KV]


def pack(core, keys, values, segments):
    msg = jax.ShapeDtypeStruct((MSG_ROWS, 2 * HALF_KV), jnp.bfloat16)
    return pl.pallas_call(
        pack_kernel,
        grid_spec=pltpu.PrefetchScalarGridSpec(
            num_scalar_prefetch=1,
            grid=(1,),
            in_specs=[
                pl.BlockSpec((TOK, 512), lambda i, s: (0, 0)),
                pl.BlockSpec((TOK, 512), lambda i, s: (0, 0)),
                pl.BlockSpec((1, TOK), lambda i, s: (0, 0)),
            ],
            out_specs=[
                pl.BlockSpec((MSG_ROWS, 512), lambda i, s: (0, 0)),
                pl.BlockSpec((MSG_ROWS, 512), lambda i, s: (0, 0)),
            ],
        ),
        out_shape=(msg, msg),
        name="pack",
    )(core, keys, values, segments)


def hold(array):
    return pltpu.with_memory_space_constraint(array, pltpu.VMEM)


def rows_to_cols(row):
    return jnp.transpose(jnp.broadcast_to(row, (128, TOK)))


def split_kernel(q_own, q_sib, out_ref):
    for i in range(ITEMS):
        ref = (q_own, q_sib)[i % 2]
        q = ref[:, i // 2 * 128 : (i // 2 + 1) * 128].astype(jnp.float32) * SCALE
        hi = q.astype(jnp.bfloat16)
        out_ref[i, :, :128] = hi
        out_ref[i, :, 128:] = (q - hi.astype(jnp.float32)).astype(jnp.bfloat16)


def split_queries(q_own, q_sib):
    return pl.pallas_call(
        split_kernel,
        in_specs=[IN_VMEM] * 2,
        out_specs=IN_VMEM,
        out_shape=pltpu.VMEM((ITEMS, TOK, 256), jnp.bfloat16),
        compiler_params=LEAN,
        name="split_queries",
    )(hold(q_own), hold(q_sib))


def seg_row(ref):
    return ref[TOK : TOK + 1, :TOK].astype(jnp.float32)


def columns(refs, first, g):
    at = pl.ds(pl.multiple_of(first + g * 128, 128), 128)
    return jnp.concatenate([r[:TOK, at] for r in refs], axis=0)


def scores(q, kv_refs, g):
    keys = columns(kv_refs, 0, g)
    keys = jnp.concatenate([keys, keys], axis=1)
    return lax.dot_general(q, keys, (((1,), (1,)), ((), ())), preferred_element_type=jnp.float32)


def weighted(p, kv_refs, g):
    vals = columns(kv_refs, HALF_KV, g)
    vals = jnp.concatenate([vals, jnp.ones_like(vals)], axis=1)
    return jnp.dot(p, vals, preferred_element_type=jnp.float32)


def fill_bias(bias_ref, place_ref, qmsg_refs, kv_refs, back):
    chip, core = place_ref[0], place_ref[1]
    side = (1 - 2 * core) * TOK
    qi = lax.broadcasted_iota(jnp.int32, (TOK, 128), 0)
    kj = lax.broadcasted_iota(jnp.int32, (TOK, 128), 1)
    dist = kj - qi
    for half in range(2):
        qseg = rows_to_cols(seg_row(qmsg_refs[half]))
        for t in range(2 * len(kv_refs)):
            b = t // 2
            k = back[b // 2]
            delta = (b % 2 - half) * side - 512 * k + (t % 2) * 128
            delta = jnp.where(chip >= k, delta, FAR)
            kseg = seg_row(kv_refs[b])[:, t % 2 * 128 : (t % 2 + 1) * 128]
            ok = (dist <= -delta) & (dist > -WINDOW - delta) & (kseg == qseg)
            bias_ref[half, :, t * 128 : (t + 1) * 128] = jnp.where(ok, 0.0, NEG)


def attend_kernel(back, init, place_ref, *refs):
    n = 2 * len(back)
    q_ref, *refs = refs
    qmsg_refs, kv_refs, refs = refs[:2], refs[2 : 2 + n], refs[2 + n :]
    if init:
        m_ref, acc_ref, p_ref, bias_ref = refs
    else:
        m_ref, acc_in, acc_ref, p_ref, bias_ref = refs
    tiles = 2 * n

    def exponents(i, slot, masked):
        g = i // (2 * GROUP)
        q = q_ref[i]
        s = scores(q, kv_refs, g)
        if init:
            own = columns([kv_refs[slot]], 0, g).astype(jnp.float32)
            both = q[:, :128].astype(jnp.float32) + q[:, 128:].astype(jnp.float32)
            m = jnp.broadcast_to(jnp.sum(own * both, axis=1, keepdims=True), (TOK, 128))
            m_ref[i] = m
        else:
            m = m_ref[i]
        for t in range(tiles):
            at = slice(t * 128, (t + 1) * 128)
            tile = s[:, at] - m
            if masked:
                tile = tile + bias_ref[slot, :, at]
            p_ref[slot, :, at] = jnp.exp2(tile).astype(jnp.bfloat16)

    def weigh(i, slot):
        acc = weighted(p_ref[slot], kv_refs, i // (2 * GROUP))
        acc_ref[i] = acc if init else acc_in[i] + acc

    def run(masked):
        if masked:
            fill_bias(bias_ref, place_ref, qmsg_refs, kv_refs, back)
        exponents(0, 0, masked)

        def body(j, _):
            for u in range(UNROLL):
                t = UNROLL * j + u
                exponents(t + 1, (u + 1) % 2, masked)
                weigh(t, u % 2)
            return 0

        lax.fori_loop(0, ITEMS // UNROLL - 1, body, 0)
        for t in range(ITEMS - UNROLL, ITEMS - 1):
            exponents(t + 1, (t + 1) % 2, masked)
            weigh(t, t % 2)
        weigh(ITEMS - 1, 1)

    if min(back) == 0:
        run(True)
        return
    low = high = seg_row(kv_refs[0])
    for ref in kv_refs[1:]:
        low, high = jnp.minimum(low, seg_row(ref)), jnp.maximum(high, seg_row(ref))
    rows = seg_row(qmsg_refs[0]), seg_row(qmsg_refs[1])
    q_low, q_high = jnp.min(jnp.minimum(*rows)), jnp.max(jnp.maximum(*rows))
    live = jnp.max(high) >= q_low
    if max(back) < 8:
        whole = (jnp.min(low) == q_high) & (place_ref[0] >= max(back))
        pl.when(whole)(lambda: run(False))
        live = live & jnp.logical_not(whole)
    pl.when(live)(lambda: run(True))


def attend(place, q2, qmsg, kv, back, state):
    init = state is None
    args = [q2, *qmsg, *kv] + ([] if init else list(state))
    m_shape = pltpu.VMEM((ITEMS, TOK, 128), jnp.float32)
    acc_shape = pltpu.VMEM((ITEMS, TOK, 256), jnp.float32)
    out_shape = (m_shape, acc_shape) if init else (acc_shape,)
    size = ITEMS * TOK * TOK * len(kv)
    out = pl.pallas_call(
        lambda *refs: attend_kernel(back, init, *refs),
        in_specs=[pl.BlockSpec(memory_space=pltpu.SMEM)] + [IN_VMEM] * len(args),
        out_specs=[IN_VMEM] * len(out_shape),
        out_shape=out_shape,
        input_output_aliases={} if init else {len(args): 0},
        scratch_shapes=[
            pltpu.VMEM((2, TOK, TOK * len(kv)), jnp.bfloat16),
            pltpu.VMEM((2, TOK, TOK * len(kv)), jnp.float32),
        ],
        cost_estimate=pl.CostEstimate(flops=size * 1024, transcendentals=size, bytes_accessed=0),
        compiler_params=LEAN,
        name="attend_" + "_".join(map(str, back)),
    )(place, *map(hold, args))
    return out if init else (state[0], out[0])


def finish_kernel(backs, place_ref, *refs):
    n = 2 * len(backs)
    q_ref, *refs = refs
    qmsg_refs, kv_refs, refs = refs[:2], refs[2 : 2 + n], refs[2 + n :]
    m_ref, acc_ref, o_own, o_sib, l_own, l_sib, worst_ref, top_ref, sum_ref, bias_ref = refs
    o_refs, lse_refs = (o_own, o_sib), (l_own, l_sib)

    def emit(h, half, m, acc):
        total = acc[:, 128:]
        at = pl.ds(pl.multiple_of(h * 128, 128), 128)
        o_refs[half][:, at] = (acc[:, :128] / total).astype(jnp.bfloat16)
        lse = LN2 * (m + jnp.log2(total))
        lse_refs[half][pl.ds(h, 1), :] = jnp.transpose(lse)[:1, :]
        return total

    worst_ref[...] = jnp.zeros_like(worst_ref)

    def item(h, _):
        for half in range(2):
            total = emit(h, half, m_ref[2 * h + half], acc_ref[2 * h + half])
            worst_ref[...] = jnp.maximum(worst_ref[...], total)
        return 0

    lax.fori_loop(0, MY_Q, item, 0)

    @pl.when(jnp.logical_not(jnp.max(worst_ref[...]) < LIMIT))
    def _():
        for b, k in enumerate(backs):
            pair = kv_refs[2 * b : 2 * b + 2]
            fill_bias(bias_ref, place_ref, qmsg_refs, pair, (k,))

            def item(h, _, b=b, pair=pair):
                for half in range(2):
                    i, g = 2 * h + half, h // GROUP
                    s = scores(q_ref[i], pair, g) + bias_ref[half]
                    top = jnp.max(s, axis=1, keepdims=True)
                    old = top_ref[i][:, :1] if b else top
                    m = jnp.maximum(old, top)
                    p = jnp.exp2(s - m).astype(jnp.bfloat16)
                    acc = weighted(p, pair, g)
                    if b:
                        acc = sum_ref[i] * jnp.exp2(old - m) + acc
                    top_ref[i] = jnp.broadcast_to(m, (TOK, 128))
                    sum_ref[i] = acc
                return 0

            lax.fori_loop(0, MY_Q, item, 0)

        def last(h, _):
            for half in range(2):
                emit(h, half, top_ref[2 * h + half], sum_ref[2 * h + half])
            return 0

        lax.fori_loop(0, MY_Q, last, 0)


def finish(place, q2, qmsg, kv, backs, state):
    args = [q2, *qmsg, *kv, *state]
    out_shape = [pltpu.VMEM((TOK, HALF_Q), jnp.bfloat16)] * 2
    out_shape += [pltpu.VMEM((MY_Q, TOK), jnp.float32)] * 2
    return pl.pallas_call(
        lambda *refs: finish_kernel(backs, *refs),
        in_specs=[pl.BlockSpec(memory_space=pltpu.SMEM)] + [IN_VMEM] * len(args),
        out_specs=[IN_VMEM] * 4,
        out_shape=out_shape,
        scratch_shapes=[
            pltpu.VMEM((TOK, 128), jnp.float32),
            pltpu.VMEM((ITEMS, TOK, 128), jnp.float32),
            pltpu.VMEM((ITEMS, TOK, 256), jnp.float32),
            pltpu.VMEM((2, TOK, 2 * TOK), jnp.float32),
        ],
        compiler_params=LEAN,
        name="finish",
    )(place, *map(hold, args))


def chips_on(by, cross=False):
    flip = 1 if cross else 0
    return [(d, (d + 2 * by) % N_DEV ^ flip) for d in range(N_DEV)]


def on_device(queries, key_rows, value_rows, segments):
    device = lax.axis_index(GRP_SEQ)
    core = device % 2
    chip = device // 2
    place = jnp.stack([chip, core]).astype(jnp.int32)
    swap = [(d, d ^ 1) for d in range(N_DEV)]

    def move(array, pairs):
        return lax.ppermute(array, GRP_SEQ, pairs)

    same, cross = pack(core[None].astype(jnp.int32), key_rows, value_rows, segments[None, :])
    fwd = [move(same, chips_on(1)), move(cross, chips_on(1, True))]
    bwd = [move(same, chips_on(8)), move(cross, chips_on(8, True))]
    sib = move(cross, swap)
    q_low, q_high = queries[:, :HALF_Q], queries[:, HALF_Q:]
    q_mine = jnp.where(core == 0, q_low, q_high)
    q_sib = move(jnp.where(core == 0, q_high, q_low), swap)
    q, qmsg = split_queries(q_mine, q_sib), [same, sib]

    state = attend(place, q, qmsg, [same, sib], (0,), None)
    seen, backs = [same, sib], [0]
    for step in range(1, 5):
        if step < 4:
            fwd_next = [move(x, chips_on(1)) for x in fwd]
            bwd_next = [move(x, chips_on(-1)) for x in bwd]
        far = 8 if step == 1 else 9 - step
        state = attend(place, q, qmsg, [*fwd, *bwd], (step, far), state)
        seen, backs = [*seen, *fwd, *bwd], [*backs, step, far]
        if step < 4:
            fwd, bwd = fwd_next, bwd_next

    o_mine, o_sib, l_mine, l_sib = finish(place, q, qmsg, seen, backs, state)
    o_other = move(o_sib, swap)
    l_other = move(l_sib, swap)
    first = core == 0
    attended = jnp.concatenate(
        [jnp.where(first, o_mine, o_other), jnp.where(first, o_other, o_mine)], axis=1
    )
    log_sums = jnp.concatenate(
        [jnp.where(first, l_mine, l_other), jnp.where(first, l_other, l_mine)], axis=0
    )
    return (attended, log_sums)


def solution(mesh):
    split = Mesh(
        mesh.devices.reshape(mesh.shape["grp"], 4, 8, 2), ("grp", "seq_0", "seq_1", "seq_2")
    )
    placed = (P(GRP_SEQ, None), P(GRP_SEQ, None), P(GRP_SEQ, None), P(GRP_SEQ))
    return jax.shard_map(
        on_device,
        mesh=split,
        in_specs=placed,
        out_specs=(P(GRP_SEQ, None), P(None, GRP_SEQ)),
        check_vma=False,
    )
```

```python
import math

import jax
import jax.numpy as jnp
from jax import lax
from jax.experimental import pallas as pl
from jax.experimental.pallas import tpu as pltpu
from jax.sharding import Mesh
from jax.sharding import PartitionSpec as P

Q_HEADS = 16
KV_HEADS = 4
HEAD_DIM = 128
WINDOW = 4096
TOK = 256
MY_Q = 8
GROUP = 4
HALF_Q = MY_Q * HEAD_DIM
HALF_KV = 2 * HEAD_DIM
MSG_ROWS = TOK + 8
GRP_SEQ = ("grp", "seq_0", "seq_1", "seq_2")
N_DEV = 256
SCALE = math.log2(math.e) / math.sqrt(HEAD_DIM)
LN2 = math.log(2.0)
NEG = -1e30
LIMIT = 2.0**100
UNROLL = 4
HP = 1
ROWS = HP * TOK
ITEMS = 2 * MY_Q // HP
PER_GROUP = 2 * GROUP // HP
IN_VMEM = pl.BlockSpec(memory_space=pltpu.VMEM)
LEAN = pltpu.CompilerParams(vmem_limit_bytes=16 << 20)
FAR = 1 << 20


def pack_kernel(core_ref, k_ref, v_ref, seg_ref, same_ref, cross_ref):
    core = core_ref[0]
    seg = jnp.broadcast_to(seg_ref[...].astype(jnp.float32), (8, TOK)).astype(jnp.bfloat16)
    seg = jnp.concatenate([seg, seg], axis=1)
    same_ref[TOK:, :] = seg
    cross_ref[TOK:, :] = seg
    for e in range(2):

        @pl.when(core == e)
        def _():
            for ref, h in ((same_ref, e), (cross_ref, 1 - e)):
                ref[:TOK, :HALF_KV] = k_ref[:, h * HALF_KV : (h + 1) * HALF_KV]
                ref[:TOK, HALF_KV:] = v_ref[:, h * HALF_KV : (h + 1) * HALF_KV]


def pack(core, keys, values, segments):
    msg = pltpu.VMEM((MSG_ROWS, 2 * HALF_KV), jnp.bfloat16)
    return pl.pallas_call(
        pack_kernel,
        in_specs=[pl.BlockSpec(memory_space=pltpu.SMEM)] + [IN_VMEM] * 3,
        out_specs=[IN_VMEM] * 2,
        out_shape=(msg, msg),
        compiler_params=LEAN,
        name="pack",
    )(core, keys, values, segments)


def hold(array):
    return pltpu.with_memory_space_constraint(array, pltpu.VMEM)


def rows_to_cols(row):
    return jnp.transpose(jnp.broadcast_to(row, (128, TOK)))


def split_kernel(q_own, q_sib, out_ref):
    for h in range(MY_Q):
        for half, ref in enumerate((q_own, q_sib)):
            i, rows = 2 * (h // HP) + half, pl.ds(h % HP * TOK, TOK)
            q = ref[:, h * 128 : (h + 1) * 128].astype(jnp.float32) * SCALE
            hi = q.astype(jnp.bfloat16)
            out_ref[i, rows, :128] = hi
            out_ref[i, rows, 128:] = (q - hi.astype(jnp.float32)).astype(jnp.bfloat16)


def split_queries(q_own, q_sib):
    return pl.pallas_call(
        split_kernel,
        in_specs=[IN_VMEM] * 2,
        out_specs=IN_VMEM,
        out_shape=pltpu.VMEM((ITEMS, ROWS, 256), jnp.bfloat16),
        compiler_params=LEAN,
        name="split_queries",
    )(hold(q_own), hold(q_sib))


def seg_row(ref):
    return ref[TOK : TOK + 1, :TOK].astype(jnp.float32)


def columns(refs, first, g):
    at = pl.ds(pl.multiple_of(first + g * 128, 128), 128)
    return jnp.concatenate([r[:TOK, at] for r in refs], axis=0)


def scores(q, kv_refs, g):
    keys = columns(kv_refs, 0, g)
    keys = jnp.concatenate([keys, keys], axis=1)
    return lax.dot_general(q, keys, (((1,), (1,)), ((), ())), preferred_element_type=jnp.float32)


def weighted(p, kv_refs, g):
    vals = columns(kv_refs, HALF_KV, g)
    vals = jnp.concatenate([vals, jnp.ones_like(vals)], axis=1)
    return jnp.dot(p, vals, preferred_element_type=jnp.float32)


def fill_bias(bias_ref, place_ref, qmsg_refs, kv_refs, blocks):
    chip, core = place_ref[0], place_ref[1]
    side = (1 - 2 * core) * TOK
    qi = lax.broadcasted_iota(jnp.int32, (TOK, 128), 0)
    kj = lax.broadcasted_iota(jnp.int32, (TOK, 128), 1)
    dist = kj - qi
    for half in range(2):
        qseg = rows_to_cols(seg_row(qmsg_refs[half]))
        for t in range(2 * len(kv_refs)):
            b = t // 2
            k, other = blocks[b]
            delta = (other - half) * side - 512 * k + (t % 2) * 128
            delta = jnp.where(chip >= k, delta, FAR)
            kseg = seg_row(kv_refs[b])[:, t % 2 * 128 : (t % 2 + 1) * 128]
            ok = (dist <= -delta) & (dist > -WINDOW - delta) & (kseg == qseg)
            bias_ref[half, :, t * 128 : (t + 1) * 128] = jnp.where(ok, 0.0, NEG)


def attend_kernel(blocks, init, place_ref, *refs):
    n = len(blocks)
    q_ref, *refs = refs
    qmsg_refs, kv_refs, refs = refs[:2], refs[2 : 2 + n], refs[2 + n :]
    if init:
        m_ref, acc_ref, p_ref, bias_ref = refs
    else:
        m_ref, acc_in, acc_ref, p_ref, bias_ref = refs
    tiles = 2 * n

    def exponents(i, slot):
        g = i // PER_GROUP
        q = q_ref[i]
        s = scores(q, kv_refs, g)
        if init:
            own = columns([kv_refs[slot]], 0, g).astype(jnp.float32)
            own = jnp.concatenate([own] * HP, axis=0)
            both = q[:, :128].astype(jnp.float32) + q[:, 128:].astype(jnp.float32)
            m = jnp.broadcast_to(jnp.sum(own * both, axis=1, keepdims=True), (ROWS, 128))
            m_ref[i] = m
        else:
            m = m_ref[i]
        for t in range(tiles):
            at = slice(t * 128, (t + 1) * 128)
            tile = s[:, at] - m + jnp.concatenate([bias_ref[slot, :, at]] * HP, axis=0)
            p_ref[slot, :, at] = jnp.exp2(tile).astype(jnp.bfloat16)

    def weigh(i, slot):
        acc = weighted(p_ref[slot], kv_refs, i // PER_GROUP)
        acc_ref[i] = acc if init else acc_in[i] + acc

    def run():
        fill_bias(bias_ref, place_ref, qmsg_refs, kv_refs, blocks)
        exponents(0, 0)

        def body(j, _):
            for u in range(UNROLL):
                t = UNROLL * j + u
                nxt = t + 1 if u < UNROLL - 1 else jnp.minimum(t + 1, ITEMS - 2)
                exponents(nxt, (u + 1) % 2)
                weigh(t, u % 2)
            return 0

        lax.fori_loop(0, ITEMS // UNROLL, body, 0)

    if init:
        run()
        return
    high = seg_row(kv_refs[0])
    for ref in kv_refs[1:]:
        high = jnp.maximum(high, seg_row(ref))
    low = jnp.minimum(seg_row(qmsg_refs[0]), seg_row(qmsg_refs[1]))
    pl.when(jnp.max(high) >= jnp.min(low))(run)


def attend(place, q2, qmsg, kv, blocks, state):
    init = state is None
    args = [q2, *qmsg, *kv] + ([] if init else list(state))
    m_shape = pltpu.VMEM((ITEMS, ROWS, 128), jnp.float32)
    acc_shape = pltpu.VMEM((ITEMS, ROWS, 256), jnp.float32)
    out_shape = (m_shape, acc_shape) if init else (acc_shape,)
    size = ITEMS * ROWS * TOK * len(kv)
    out = pl.pallas_call(
        lambda *refs: attend_kernel(blocks, init, *refs),
        in_specs=[pl.BlockSpec(memory_space=pltpu.SMEM)] + [IN_VMEM] * len(args),
        out_specs=[IN_VMEM] * len(out_shape),
        out_shape=out_shape,
        input_output_aliases={} if init else {len(args): 0},
        scratch_shapes=[
            pltpu.VMEM((2, ROWS, TOK * len(kv)), jnp.bfloat16),
            pltpu.VMEM((2, TOK, TOK * len(kv)), jnp.float32),
        ],
        cost_estimate=pl.CostEstimate(flops=size * 128, transcendentals=0, bytes_accessed=0),
        compiler_params=LEAN,
        name="attend_" + "_".join(f"{k}{'so'[o]}" for k, o in blocks),
    )(place, *map(hold, args))
    return out if init else (state[0], out[0])


def finish_kernel(backs, place_ref, *refs):
    n = 2 * len(backs)
    q_ref, *refs = refs
    qmsg_refs, kv_refs, refs = refs[:2], refs[2 : 2 + n], refs[2 + n :]
    m_ref, acc_ref, o_own, o_sib, l_own, l_sib, worst_ref, top_ref, sum_ref, bias_ref = refs
    o_refs, lse_refs = (o_own, o_sib), (l_own, l_sib)

    def emit(h, half, m, acc):
        total = acc[:, 128:]
        at = pl.ds(pl.multiple_of(h * 128, 128), 128)
        o_refs[half][:, at] = (acc[:, :128] / total).astype(jnp.bfloat16)
        lse = LN2 * (m + jnp.log2(total))
        lse_refs[half][pl.ds(h, 1), :] = jnp.transpose(lse)[:1, :]
        return total

    worst_ref[...] = jnp.zeros_like(worst_ref)

    def place_of(p, j):
        return p * HP + j, pl.ds(j * TOK, TOK)

    def item(p, _):
        for half in range(2):
            for j in range(HP):
                h, rows = place_of(p, j)
                total = emit(h, half, m_ref[2 * p + half, rows], acc_ref[2 * p + half, rows])
                worst_ref[...] = jnp.maximum(worst_ref[...], total)
        return 0

    lax.fori_loop(0, MY_Q // HP, item, 0)

    @pl.when(jnp.logical_not(jnp.max(worst_ref[...]) < LIMIT))
    def _():
        for b, k in enumerate(backs):
            pair = kv_refs[2 * b : 2 * b + 2]
            fill_bias(bias_ref, place_ref, qmsg_refs, pair, ((k, 0), (k, 1)))

            def item(p, _, b=b, pair=pair):
                for half in range(2):
                    for j in range(HP):
                        h, rows = place_of(p, j)
                        i, g = 2 * p + half, p * HP // GROUP
                        s = scores(q_ref[i, rows], pair, g) + bias_ref[half]
                        top = jnp.max(s, axis=1, keepdims=True)
                        old = top_ref[i, rows][:, :1] if b else top
                        m = jnp.maximum(old, top)
                        w = jnp.exp2(s - m).astype(jnp.bfloat16)
                        acc = weighted(w, pair, g)
                        if b:
                            acc = sum_ref[i, rows] * jnp.exp2(old - m) + acc
                        top_ref[i, rows] = jnp.broadcast_to(m, (TOK, 128))
                        sum_ref[i, rows] = acc
                return 0

            lax.fori_loop(0, MY_Q // HP, item, 0)

        def last(p, _):
            for half in range(2):
                for j in range(HP):
                    h, rows = place_of(p, j)
                    emit(h, half, top_ref[2 * p + half, rows], sum_ref[2 * p + half, rows])
            return 0

        lax.fori_loop(0, MY_Q // HP, last, 0)


def finish(place, q2, qmsg, kv, backs, state):
    args = [q2, *qmsg, *kv, *state]
    out_shape = [pltpu.VMEM((TOK, HALF_Q), jnp.bfloat16)] * 2
    out_shape += [pltpu.VMEM((MY_Q, TOK), jnp.float32)] * 2
    return pl.pallas_call(
        lambda *refs: finish_kernel(backs, *refs),
        in_specs=[pl.BlockSpec(memory_space=pltpu.SMEM)] + [IN_VMEM] * len(args),
        out_specs=[IN_VMEM] * 4,
        out_shape=out_shape,
        scratch_shapes=[
            pltpu.VMEM((TOK, 128), jnp.float32),
            pltpu.VMEM((ITEMS, ROWS, 128), jnp.float32),
            pltpu.VMEM((ITEMS, ROWS, 256), jnp.float32),
            pltpu.VMEM((2, TOK, 2 * TOK), jnp.float32),
        ],
        compiler_params=LEAN,
        name="finish",
    )(place, *map(hold, args))


def at(d):
    return d // 64, d // 16 % 4, d // 2 % 8, d % 2


def ring(send, cross=False):
    pairs = []
    for d in range(N_DEV):
        y, x, z, core = at(d)
        chip = send(y, x, z, d // 2)
        if chip is not None and 0 <= chip < N_DEV // 2:
            pairs.append((d, 2 * chip + (core ^ 1 if cross else core)))
    return pairs


def onward(y, x, z, chip):
    return chip + 1


def eight_on(y, x, z, chip):
    return None if z == 0 else chip + 8 if chip < 120 else chip - 120 if z < 3 else None


def first_back(y, x, z, chip):
    return chip + 7 if z == 0 else chip - 1


def back(y, x, z, chip):
    return (chip - 1) % (N_DEV // 2)


def around(y, x, z, chip):
    return 32 * y + 8 * ((x - 1) % 4) if z == 0 else None


def around_last(y, x, z, chip):
    return None if z else 32 * (y + 1) if x == 1 else around(y, x, z, chip)


def on_device(queries, key_rows, value_rows, segments):
    device = lax.axis_index(GRP_SEQ)
    core = device % 2
    chip = device // 2
    place = jnp.stack([chip, core]).astype(jnp.int32)
    swap = [(d, d ^ 1) for d in range(N_DEV)]

    def move(array, pairs):
        return lax.ppermute(array, GRP_SEQ, pairs)

    bottom = chip % 8 == 0
    same, cross = pack(core[None].astype(jnp.int32), key_rows, value_rows, segments[None, :])
    fwd = [move(same, ring(onward)), move(cross, ring(onward, True))]
    bwd = [move(same, ring(eight_on)), move(cross, ring(eight_on, True))]
    sib = move(cross, swap)
    late = [move(same, ring(around)), move(cross, ring(around, True))]
    q_low, q_high = queries[:, :HALF_Q], queries[:, HALF_Q:]
    q_mine = jnp.where(core == 0, q_low, q_high)
    q_sib = move(jnp.where(core == 0, q_high, q_low), swap)
    q, mine = split_queries(q_mine, q_sib), [same, sib]

    tie = lax.optimization_barrier
    state = None
    hop, seen = bwd, [*mine]
    for step in range(1, 5):
        far = 9 - step
        if state is not None:
            (fwd[0], bwd[0], acc) = tie((fwd[0], bwd[0], state[1]))
            state = (state[0], acc)
        if step < 3:
            fwd[1], bwd[1], late[0], late[1] = tie((fwd[1], bwd[1], late[0], late[1]))
        here = [*fwd, *bwd] if step > 1 else [*mine, *fwd]
        if step == 1:
            hop = bwd
            bwd = [jnp.where(bottom, m, x) for m, x in zip(mine, bwd)]
        blocks = [(k, o) for k in ((step, far) if step > 1 else (0, 1)) for o in range(2)]
        seen = [*seen, *(here if step > 1 else fwd)]
        if step < 4:
            turn = first_back if step == 1 else back
            moved = [(move(f, ring(onward)), move(b, ring(turn))) for f, b in zip(fwd, bwd)]
            fwd, bwd = [m[0] for m in moved], [m[1] for m in moved]
            if step < 3:
                late = [move(x, ring(around if step == 1 else around_last)) for x in late]
            state = attend(place, q, mine, here, tuple(blocks), state)
        if step == 3:
            late[0], late[1], acc = tie((late[0], late[1], state[1]))
            hop = [jnp.where(bottom, m, x) for m, x in zip(late, hop)]
            state = attend(place, q, mine, hop, ((8, 0), (8, 1)), (state[0], acc))
        if step == 4:
            for o in range(2):
                state = attend(place, q, mine, here[o::2], tuple(blocks[o::2]), state)
    backs = [0, 1, 2, 7, 3, 6, 4, 5, 8]
    seen = [*seen, *hop]

    o_mine, o_sib, l_mine, l_sib = finish(place, q, mine, seen, backs, state)
    o_other = move(o_sib, swap)
    l_other = move(l_sib, swap)
    first = core == 0
    attended = jnp.concatenate(
        [jnp.where(first, o_mine, o_other), jnp.where(first, o_other, o_mine)], axis=1
    )
    log_sums = jnp.concatenate(
        [jnp.where(first, l_mine, l_other), jnp.where(first, l_other, l_mine)], axis=0
    )
    return (attended, log_sums)


def solution(mesh):
    split = Mesh(
        mesh.devices.reshape(mesh.shape["grp"], 4, 8, 2), ("grp", "seq_0", "seq_1", "seq_2")
    )
    placed = (P(GRP_SEQ, None), P(GRP_SEQ, None), P(GRP_SEQ, None), P(GRP_SEQ))
    return jax.shard_map(
        on_device,
        mesh=split,
        in_specs=placed,
        out_specs=(P(GRP_SEQ, None), P(None, GRP_SEQ)),
        check_vma=False,
    )
```
